32 devices in a mesh: dp: 4 (over y, z), sp: 8 (over x, core).
Axes of the slice: x: 4, y: 2, z: 2, core: 2. Of those that a mesh axis runs over, the one named last changes fastest.
The devices are a block of a 4x4x8 slice.
Arguments:
- latent: bfloat16 [64, 8, 192, 640], P('dp', 'sp'), parts along dimension 0
- time_emb: bfloat16 [64, 1280], P('dp'), parts along dimension 0
- context: bfloat16 [64, 77, 768], P('dp'), parts along dimension 0
- res_conv: bfloat16 [2, 2, 3, 3, 640, 640], replicated
- res_time: bfloat16 [2, 1280, 640], replicated
- res_norm: bfloat16 [2, 2, 2, 32, 20], replicated
- attn_norm: bfloat16 [2, 32, 20], replicated
- proj_inout: bfloat16 [2, 640, 640], replicated
- self_qkv: bfloat16 [3, 640, 8, 80], replicated
- self_out: bfloat16 [8, 80, 640], replicated
- cross_q: bfloat16 [640, 8, 80], replicated
- cross_kv: bfloat16 [2, 768, 8, 80], replicated
- cross_out: bfloat16 [8, 80, 640], replicated
- ff_in: bfloat16 [640, 5120], replicated
- ff_out: bfloat16 [2560, 640], replicated
Outputs:
- output: bfloat16 [64, 8, 192, 640], P('dp', 'sp'), parts along dimension 0
There are 4 independent parts. The reference program is written for one: setup_inputs(seed, part) draws one part's arguments, and reference() takes and returns one part's arrays. A program takes and returns all parts, laid end to end along the dimension named above; an argument that names none is the same for every part.
All inputs are finite; a program needn't handle non-finite values.
Results may differ from the reference program's by a relative error of at most 0.0135156.
Values are sent between devices in bfloat16 or wider.
A program may use at most 768 MiB of HBM per device.

```python
import math
import jax
import jax.numpy as jnp
from jax import lax

BATCH = 16
BANDS = 8
BAND_ROWS = 1
WIDTH = 192
CHANNELS = 640
GROUPS = 32
HEADS = 8
TEXT = 77
TEXT_DIM = 768
TIME_DIM = 1280

HEIGHT = BANDS * BAND_ROWS
TOKENS = HEIGHT * WIDTH
BAND_TOKENS = BAND_ROWS * WIDTH
HEAD_DIM = CHANNELS // HEADS
GROUP_WIDTH = CHANNELS // GROUPS
GN_EPS = 1e-6
LN_EPS = 1e-5


def normal_weight(rng_key, out_shape, std_scale):
    return (jax.random.normal(rng_key, out_shape, jnp.float32) * std_scale).astype(jnp.bfloat16)


def norm_params(rng_key, lead_shape):
    spread = 0.4 * jax.random.normal(rng_key, lead_shape + (2, GROUPS, GROUP_WIDTH), jnp.float32)
    offset = jnp.array([1.0, 0.0], jnp.float32)[:, None, None]
    return (spread + offset).astype(jnp.bfloat16)


def setup_inputs(seed: int = 0, part: int = 0) -> dict:
    part_keys = jax.random.split(jax.random.fold_in(jax.random.key(seed), part), 5)
    weight_keys = jax.random.split(jax.random.key(seed + 1), 12)
    rows_pos = (jnp.arange(HEIGHT, dtype=jnp.float32) + 0.5) / HEIGHT
    wave_phase = jax.random.uniform(part_keys[0], (BATCH, 1, 1, 1), jnp.float32, 0.0, 2.0 * math.pi)
    loading = 1.0 + 0.5 * jax.random.normal(part_keys[1], (BATCH, 1, 1, CHANNELS), jnp.float32)
    row_wave = jnp.cos(math.pi * rows_pos[None, :, None, None] + wave_phase)
    white_noise = jax.random.normal(part_keys[2], (BATCH, HEIGHT, WIDTH, CHANNELS), jnp.float32)
    self_sharp = math.sqrt(math.log(TOKENS))
    cross_sharp = math.sqrt(math.log(TEXT))
    chan_scale = CHANNELS ** -0.5
    qkv_scale = chan_scale * jnp.array([self_sharp, 1.0, 1.0], jnp.float32)[:, None, None, None]
    return {
        'latent': (white_noise + 1.5 * row_wave * loading).astype(jnp.bfloat16),
        'time_emb': jax.random.normal(part_keys[3], (BATCH, TIME_DIM), jnp.float32).astype(jnp.bfloat16),
        'context': jax.random.normal(part_keys[4], (BATCH, TEXT, TEXT_DIM), jnp.float32).astype(jnp.bfloat16),
        'res_conv': normal_weight(weight_keys[0], (2, 2, 3, 3, CHANNELS, CHANNELS), (9 * CHANNELS) ** -0.5),
        'res_time': normal_weight(weight_keys[1], (2, TIME_DIM, CHANNELS), TIME_DIM ** -0.5),
        'res_norm': norm_params(weight_keys[2], (2, 2)),
        'attn_norm': norm_params(weight_keys[3], ()),
        'proj_inout': normal_weight(weight_keys[4], (2, CHANNELS, CHANNELS), chan_scale),
        'self_qkv': normal_weight(weight_keys[5], (3, CHANNELS, HEADS, HEAD_DIM), qkv_scale),
        'self_out': normal_weight(weight_keys[6], (HEADS, HEAD_DIM, CHANNELS), chan_scale),
        'cross_q': normal_weight(weight_keys[7], (CHANNELS, HEADS, HEAD_DIM), chan_scale * cross_sharp),
        'cross_kv': normal_weight(weight_keys[8], (2, TEXT_DIM, HEADS, HEAD_DIM), TEXT_DIM ** -0.5),
        'cross_out': normal_weight(weight_keys[9], (HEADS, HEAD_DIM, CHANNELS), chan_scale),
        'ff_in': normal_weight(weight_keys[10], (CHANNELS, 8 * CHANNELS), chan_scale),
        'ff_out': normal_weight(weight_keys[11], (4 * CHANNELS, CHANNELS), (4 * CHANNELS) ** -0.5),
    }


def group_norm(hidden, scale_shift):
    feat_f32 = hidden.astype(jnp.float32).reshape(BATCH, TOKENS, GROUPS, GROUP_WIDTH)
    grp_mean = jnp.mean(feat_f32, axis=(1, 3), keepdims=True)
    grp_msq = jnp.mean(feat_f32 * feat_f32, axis=(1, 3), keepdims=True)
    normed = (feat_f32 - grp_mean) * lax.rsqrt(grp_msq - grp_mean * grp_mean + GN_EPS)
    normed = normed * scale_shift[0].astype(jnp.float32) + scale_shift[1].astype(jnp.float32)
    return normed.reshape(BATCH, HEIGHT, WIDTH, CHANNELS)


def conv_same(act_in, kernel):
    return lax.conv_general_dilated(act_in.astype(jnp.float32), kernel.astype(jnp.float32), (1, 1), 'SAME', dimension_numbers=('NHWC', 'HWIO', 'NHWC'))


def res_block(hidden, time_emb, kernels, time_weight, norm_pair):
    act_one = jax.nn.silu(group_norm(hidden, norm_pair[0])).astype(jnp.bfloat16)
    time_act = jax.nn.silu(time_emb.astype(jnp.float32)).astype(jnp.bfloat16)
    time_proj = jnp.dot(time_act, time_weight, preferred_element_type=jnp.float32)
    mid_act = (conv_same(act_one, kernels[0]) + time_proj[:, None, None, :]).astype(jnp.bfloat16)
    act_two = jax.nn.silu(group_norm(mid_act, norm_pair[1])).astype(jnp.bfloat16)
    return (hidden.astype(jnp.float32) + conv_same(act_two, kernels[1])).astype(jnp.bfloat16)


def layer_norm(tokens):
    feat_f32 = tokens.astype(jnp.float32)
    centred = feat_f32 - jnp.mean(feat_f32, axis=-1, keepdims=True)
    return (centred * lax.rsqrt(jnp.mean(centred * centred, axis=-1, keepdims=True) + LN_EPS)).astype(jnp.bfloat16)


def project(rows_flat, weight):
    return jnp.dot(rows_flat, weight.reshape(weight.shape[0], -1), preferred_element_type=jnp.float32).astype(jnp.bfloat16)


def attend(queries, key_all, val_all):
    logits = jnp.einsum('bqhd,bkhd->bhqk', queries.astype(jnp.float32), key_all.astype(jnp.float32)) * (HEAD_DIM ** -0.5)
    row_max = jnp.max(logits, axis=-1, keepdims=True)
    weights = jnp.exp(logits - row_max)
    row_sum = jnp.sum(weights, axis=-1)
    weighted = jnp.einsum('bhqk,bkhd->bhqd', weights.astype(jnp.bfloat16).astype(jnp.float32), val_all.astype(jnp.float32))
    return (weighted / row_sum[..., None]).astype(jnp.bfloat16)


def out_project(attended, weight):
    return jnp.einsum('bhqd,hdc->bqc', attended.astype(jnp.float32), weight.astype(jnp.float32))


def transformer_block(hidden, context, attn_norm, proj_inout, self_qkv, self_out, cross_q, cross_kv, cross_out, ff_in, ff_out):
    normed = group_norm(hidden, attn_norm).astype(jnp.bfloat16).reshape(BATCH * TOKENS, CHANNELS)
    tokens = jnp.dot(normed, proj_inout[0], preferred_element_type=jnp.float32).astype(jnp.bfloat16)
    ln_tokens = layer_norm(tokens)
    key_all = project(ln_tokens, self_qkv[1]).reshape(BATCH, TOKENS, HEADS, HEAD_DIM)
    val_all = project(ln_tokens, self_qkv[2]).reshape(BATCH, TOKENS, HEADS, HEAD_DIM)
    ctx_flat = context.reshape(BATCH * TEXT, TEXT_DIM)
    ctx_key = project(ctx_flat, cross_kv[0]).reshape(BATCH, TEXT, HEADS, HEAD_DIM)
    ctx_val = project(ctx_flat, cross_kv[1]).reshape(BATCH, TEXT, HEADS, HEAD_DIM)
    flat_count = BATCH * BAND_TOKENS

    def band_step(operands):
        resid_band, tok_band, ln_band = operands
        self_query = project(ln_band.reshape(flat_count, CHANNELS), self_qkv[0]).reshape(BATCH, BAND_TOKENS, HEADS, HEAD_DIM)
        self_att = out_project(attend(self_query, key_all, val_all), self_out)
        tok_one = (tok_band.astype(jnp.float32) + self_att).astype(jnp.bfloat16)
        cross_query = project(layer_norm(tok_one).reshape(flat_count, CHANNELS), cross_q).reshape(BATCH, BAND_TOKENS, HEADS, HEAD_DIM)
        cross_att = out_project(attend(cross_query, ctx_key, ctx_val), cross_out)
        tok_two = (tok_one.astype(jnp.float32) + cross_att).astype(jnp.bfloat16).reshape(flat_count, CHANNELS)
        hidden_ff = jnp.dot(layer_norm(tok_two), ff_in, preferred_element_type=jnp.float32)
        gated_ff = (hidden_ff[:, :4 * CHANNELS] * jax.nn.gelu(hidden_ff[:, 4 * CHANNELS:], approximate=False)).astype(jnp.bfloat16)
        tok_three = (tok_two.astype(jnp.float32) + jnp.dot(gated_ff, ff_out, preferred_element_type=jnp.float32)).astype(jnp.bfloat16)
        block_out = resid_band.reshape(flat_count, CHANNELS).astype(jnp.float32) + jnp.dot(tok_three, proj_inout[1], preferred_element_type=jnp.float32)
        return block_out.astype(jnp.bfloat16).reshape(BATCH, BAND_TOKENS, CHANNELS)

    def to_bands(array_in):
        return jnp.swapaxes(array_in.reshape(BATCH, BANDS, BAND_TOKENS, CHANNELS), 0, 1)

    band_out = lax.map(band_step, (to_bands(hidden), to_bands(tokens), to_bands(ln_tokens)))
    return jnp.swapaxes(band_out, 0, 1).reshape(BATCH, HEIGHT, WIDTH, CHANNELS)


def reference(latent, time_emb, context, res_conv, res_time, res_norm, attn_norm, proj_inout, self_qkv, self_out, cross_q, cross_kv, cross_out, ff_in, ff_out):
    after_first = res_block(latent, time_emb, res_conv[0], res_time[0], res_norm[0])
    middle = transformer_block(after_first, context, attn_norm, proj_inout, self_qkv, self_out, cross_q, cross_kv, cross_out, ff_in, ff_out)
    return res_block(middle, time_emb, res_conv[1], res_time[1], res_norm[1])
```

```python
import functools
import math
import jax
import jax.numpy as jnp
from jax import lax
from jax.experimental import pallas as pl
from jax.experimental.pallas import tpu as pltpu
from jax.sharding import PartitionSpec as P

GN_EPS = 1e-6
LN_EPS = 1e-5
LANES = 128
SUBLANES = 8
MESH = pl.DeviceIdType.MESH
LOGIT_LIMIT = 60.0
VALUE_LIMIT = 1e8
MIB = 2 ** 20
F32 = jnp.float32
BF16 = jnp.bfloat16
LHS_T = (((0,), (0,)), ((), ()))
BOTH_T = (((0,), (1,)), ((), ()))


def tdot(weight, act):
    return lax.dot_general(weight, act, LHS_T, preferred_element_type=F32)


def lane_sum(parts, value):
    total = parts
    for off in range(0, value.shape[1], LANES):
        total = total + value[:, off:off + LANES]
    return total


def group_affine(sums, squares, width, count, gain, shift):
    span = math.lcm(width, SUBLANES)
    row = lax.broadcasted_iota(jnp.int32, (SUBLANES, LANES), 0)
    scales, offsets = [], []

    def group_mean(array, base, low, high):
        total = None
        for top in range(0, span, SUBLANES):
            first, last = max(low - top, 0), min(high - top, SUBLANES)
            if first < last:
                tile = array[base + top:base + top + SUBLANES]
                if last - first < SUBLANES:
                    tile = jnp.where((row >= first) & (row < last), tile, 0.0)
                total = tile if total is None else total + tile
        for turn in (4, 2, 1):
            total = total + pltpu.roll(total, turn, 0)
        return jnp.broadcast_to(jnp.sum(total, axis=1, keepdims=True), (SUBLANES, LANES)) / count

    for base in range(0, sums.shape[0], span):
        means, rstds = [], []
        for low in range(0, span, width):
            mean = group_mean(sums, base, low, low + width)
            means.append(mean)
            rstds.append(lax.rsqrt(group_mean(squares, base, low, low + width) - mean * mean + GN_EPS))
        for top in range(0, span, SUBLANES):
            mean, rstd = means[top // width], rstds[top // width]
            for nxt in range(top // width + 1, (top + SUBLANES - 1) // width + 1):
                mean = jnp.where(row >= nxt * width - top, means[nxt], mean)
                rstd = jnp.where(row >= nxt * width - top, rstds[nxt], rstd)
            here = slice(base + top, base + top + SUBLANES)
            scale = rstd * gain[here]
            scales.append(scale)
            offsets.append(shift[here] - mean * scale)
    return jnp.concatenate(scales, axis=0), jnp.concatenate(offsets, axis=0)


def affine(block, scale, offset):
    pieces = [block[:, off:off + LANES].astype(F32) * scale + offset for off in range(0, block.shape[1], LANES)]
    return jnp.concatenate(pieces, axis=1)


def silu(value):
    half = 0.5 * value
    return half + half * jnp.tanh(half)


def layer_norm(tokens):
    centred = tokens - jnp.mean(tokens, axis=0, keepdims=True)
    return (centred * lax.rsqrt(jnp.mean(centred * centred, axis=0, keepdims=True) + LN_EPS)).astype(BF16)


def res_phase(which, first, width, group_width, hid, cols, cur, wide, aff, weight, sums, squares, conv_block, turn, emit):
    channels, tokens = cur.shape
    count = float(tokens * group_width)
    gain = jnp.where(first, cols[:, 0:1], cols[:, 2:3])
    shift = jnp.where(first, cols[:, 1:2], cols[:, 3:4])
    aff[0], aff[1] = group_affine(sums, squares, group_width, count, gain, shift)
    act_block = 2 * width
    row = lax.broadcasted_iota(jnp.int32, (act_block, channels), 0)
    row = jnp.where(row >= width, row - width, row)

    def widen(i, carry):
        tok = pl.ds(pl.multiple_of(i * act_block, LANES), act_block)
        act = silu(affine(cur[:, tok], aff[0], aff[1])).T
        dst = pl.ds(pl.multiple_of(i * act_block + width, 64), act_block)
        wide[dst, 0:channels] = jnp.where(row == 0, 0.0, pltpu.roll(act, 1, 0)).astype(BF16)
        wide[dst, channels:2 * channels] = act.astype(BF16)
        wide[dst, 2 * channels:3 * channels] = jnp.where(row == width - 1, 0.0, pltpu.roll(act, act_block - 1, 0)).astype(BF16)
        return carry

    lax.fori_loop(0, tokens // act_block, widen, 0)
    if weight[1] is not None:
        weight[1].wait()
    time_term = cols[:, 4:5]

    def convolve(i, carry):
        block = lax.rem(i + turn, tokens // conv_block)
        start = block * conv_block
        tok = pl.ds(pl.multiple_of(start, LANES), conv_block)
        taps_in = jnp.concatenate([wide[pl.ds(pl.multiple_of(start + dy * width, 64), conv_block), :] for dy in range(3)], axis=1)
        value = lax.dot_general(weight[0][which], taps_in, BOTH_T, preferred_element_type=F32)
        out = value + jnp.where(first, time_term, hid[:, tok].astype(F32))
        cur[:, tok] = out.astype(BF16)
        emit(block, tok, out)
        out = out.astype(BF16).astype(F32)
        return lane_sum(carry[0], out), lane_sum(carry[1], out * out)

    zero = jnp.zeros((channels, LANES), F32)
    return lax.fori_loop(0, tokens // conv_block, convolve, (zero, zero))


def clear_border(wide, width):
    rows, taps = wide.shape
    wide[0:width, :] = jnp.zeros((width, taps), BF16)
    wide[rows - width:rows, :] = jnp.zeros((width, taps), BF16)


def weight_copies(weight_hbm, weight_scr, sems, first_conv):
    return lambda i: pltpu.make_async_copy(weight_hbm.at[first_conv + i], weight_scr.at[i], sems.at[i])


def res_in_kernel(width, group_width, first_conv, conv_block, hid_ref, cols_ref, weight_hbm, *refs):
    out_ref, parts_ref, hid_scr, wide_scr, aff_scr, weight_scr, sems = refs[-7:]
    channels, tokens = hid_scr.shape
    copies = weight_copies(weight_hbm, weight_scr, sems, first_conv)
    for i in range(2):
        copies(i).start()
    clear_border(wide_scr, width)
    act_block = 2 * width
    cur = out_ref.at[0]

    def load(i, carry):
        tok = pl.ds(pl.multiple_of(i * act_block, LANES), act_block)
        block = hid_ref[tok, :].astype(F32).T
        hid_scr[:, tok] = block.astype(BF16)
        cur[:, tok] = block.astype(BF16)
        return lane_sum(carry[0], block), lane_sum(carry[1], block * block)

    zero = jnp.zeros((channels, LANES), F32)
    stats = lax.fori_loop(0, tokens // act_block, load, (zero, zero))

    def half(which, stats):
        return res_phase(which, which == 0, width, group_width, hid_scr, cols_ref[0], cur, wide_scr, aff_scr, (weight_scr, copies(which)), *stats, conv_block, 0, lambda block, tok, out: None)

    sums, squares = lax.fori_loop(0, 2, half, stats)
    parts_ref[0, :, 0:LANES] = sums
    parts_ref[0, :, LANES:2 * LANES] = squares


def res_out_kernel(axis, bands, width, group_width, first_conv, conv_block, hid_ref, parts_ref, cols_ref, weight_hbm, out_hbm, cur_scr, wide_scr, aff_scr, rows_scr, weight_scr, sems, send_sems, recv_sems, own_sems):
    images, channels, tokens = hid_ref.shape
    band = tokens // bands
    me = lax.axis_index(axis)
    copies = weight_copies(weight_hbm, weight_scr, sems, first_conv)
    for i in range(2):
        copies(i).start()
    barrier = pltpu.get_barrier_semaphore()
    for step in range(1, bands):
        pl.semaphore_signal(barrier, inc=1, device_id={axis: lax.rem(me + step, bands)}, device_id_type=MESH)
    clear_border(wide_scr, width)
    pl.semaphore_wait(barrier, bands - 1)

    turn = lax.div(me * band, conv_block) + 1

    def remote(image, peer, source, low=0, high=band):
        return pltpu.make_async_remote_copy(
            src_ref=rows_scr.at[image, pl.ds(peer * band + low, high - low)], dst_ref=out_hbm.at[image * bands + source, pl.ds(low, high - low)],
            send_sem=send_sems.at[image, peer], recv_sem=recv_sems.at[image, source], device_id={axis: peer}, device_id_type=MESH)

    def local(image, peer, low=0, high=band):
        return pltpu.make_async_copy(rows_scr.at[image, pl.ds(peer * band + low, high - low)], out_hbm.at[image * bands + me, pl.ds(low, high - low)], own_sems.at[image])

    def per_image(image, carry):
        cur_scr[...] = hid_ref[image]

        def half(which, stats):
            def emit(block, tok, out):
                rows_scr[image, tok, :] = out.T.astype(BF16)
                for ready in range(tokens // conv_block):
                    for peer in range(bands):
                        low = max(ready * conv_block - peer * band, 0)
                        high = min((ready + 1) * conv_block - peer * band, band)
                        if low >= high:
                            continue
                        now = (which == 1) & (block == ready)

                        @pl.when(now & (me != peer))
                        def _():
                            remote(image, peer, me, low, high).start()

                        @pl.when(now & (me == peer))
                        def _():
                            local(image, peer, low, high).start()

            @pl.when((image == 0))
            def _():
                copies(which).wait()

            return res_phase(which, which == 0, width, group_width, hid_ref.at[image], cols_ref[image], cur_scr, wide_scr, aff_scr, (weight_scr, None), *stats, conv_block, turn, emit)

        lax.fori_loop(0, 2, half, (parts_ref[image, :, 0:LANES], parts_ref[image, :, LANES:2 * LANES]))
        return carry

    lax.fori_loop(0, images, per_image, 0)
    for image in range(images):
        for peer in range(bands):
            @pl.when(me != peer)
            def _():
                remote(image, peer, me).wait_send()
                remote(image, peer, peer).wait_recv()
        local(image, me).wait()


def res_cost(images, channels, tokens):
    return pl.CostEstimate(flops=2 * 2 * 9 * images * channels * channels * tokens, bytes_accessed=40 * channels * channels, transcendentals=0)


def res_block_in(image, images, hid, cols, weights, first_conv, width, group_width, before):
    tokens, channels = hid.shape
    conv_block, taps = 512, 3 * channels
    slot = lambda i: (image, 0, 0)
    any_spec = pl.BlockSpec(memory_space=pl.ANY)
    return pl.pallas_call(
        functools.partial(res_in_kernel, width, group_width, first_conv, conv_block),
        grid=(1,),
        out_shape=(jax.ShapeDtypeStruct((images, channels, tokens), BF16), jax.ShapeDtypeStruct((images, channels, 2 * LANES), F32)),
        in_specs=[pl.BlockSpec(hid.shape, lambda i: (0, 0)), pl.BlockSpec((1,) + cols.shape[1:], slot), pl.BlockSpec(memory_space=pltpu.HBM)] + [any_spec] * len(before),
        out_specs=(pl.BlockSpec((1, channels, tokens), slot), pl.BlockSpec((1, channels, 2 * LANES), slot)),
        scratch_shapes=[
            pltpu.VMEM((channels, tokens), BF16), pltpu.VMEM((tokens + 2 * width, taps), BF16),
            pltpu.VMEM((2, channels, LANES), F32), pltpu.VMEM((2, 3 * taps, channels), BF16), pltpu.SemaphoreType.DMA((2,))],
        input_output_aliases={3: 0, 4: 1} if before else {},
        name='res_in',
        cost_estimate=res_cost(1, channels, tokens),
        compiler_params=pltpu.CompilerParams(vmem_limit_bytes=62 * MIB),
    )(hid, cols, weights, *before)


def res_block_out(axis, bands, stacked, parts, cols, weights, first_conv, width, group_width):
    images, channels, tokens = stacked.shape
    conv_block, taps = 512, 3 * channels
    vmem = pl.BlockSpec(memory_space=pltpu.VMEM)
    return pl.pallas_call(
        functools.partial(res_out_kernel, axis, bands, width, group_width, first_conv, conv_block),
        out_shape=jax.ShapeDtypeStruct((images * bands, tokens // bands, channels), BF16),
        in_specs=[vmem, vmem, vmem, pl.BlockSpec(memory_space=pltpu.HBM)],
        out_specs=pl.BlockSpec(memory_space=pltpu.HBM),
        scratch_shapes=[
            pltpu.VMEM((channels, tokens), BF16), pltpu.VMEM((tokens + 2 * width, taps), BF16),
            pltpu.VMEM((2, channels, LANES), F32), pltpu.VMEM((images, tokens, channels), BF16), pltpu.VMEM((2, 3 * taps, channels), BF16),
            pltpu.SemaphoreType.DMA((2,)), pltpu.SemaphoreType.DMA((images, bands)), pltpu.SemaphoreType.DMA((images, bands)), pltpu.SemaphoreType.DMA((images,))],
        name='res_out',
        cost_estimate=res_cost(images, channels, tokens),
        compiler_params=pltpu.CompilerParams(vmem_limit_bytes=48 * MIB, collective_id=0, has_side_effects=True),
    )(stacked, parts, cols, weights)


def former_kernel(heads, text, group_width, block, q_block, k_chunk, hid_ref, part_in_ref, cols_ref, ctx_key_ref, ctx_val_ref, *refs):
    weights_hbm, refs = refs[:8], refs[8:]
    out_ref, parts_ref, tok_scr, query_scr, key_scr, val_scr, att_scr, logit_scr, prob_scr, cross_scr, gate_scr = refs[:11]
    weights, sems = refs[11:19], refs[19]
    _, channels, tokens = hid_ref.shape
    head_dim = channels // heads
    ff_width = weights[6].shape[0]
    count = float(tokens * group_width)
    exp_scale = head_dim ** -0.5 * 1.4426950408889634
    first = pl.program_id(0) == 0
    copies = [pltpu.make_async_copy(weights_hbm[i], weights[i], sems.at[i]) for i in range(8)]

    @pl.when(first)
    def _():
        for copy in copies:
            copy.start()
        query_scr[...] = jnp.zeros(query_scr.shape, BF16)

    def ready(*which):
        @pl.when(first)
        def _():
            for i in which:
                copies[i].wait()

    scale, offset = group_affine(part_in_ref[0, :, 0:LANES], part_in_ref[0, :, LANES:2 * LANES], group_width, count, cols_ref[:, 0:1], cols_ref[:, 1:2])
    ready(0, 1)
    pad = jnp.zeros((query_scr.shape[1] - head_dim, block), BF16)

    def largest(value, before):
        square = value.astype(F32)
        square = (square * square).reshape(heads, head_dim, block)
        return jnp.maximum(jnp.sum(square, axis=1), before)

    def project(i, carry):
        tok = pl.ds(pl.multiple_of(i * block, LANES), block)
        token = tdot(weights[0][...], affine(hid_ref[0, :, tok], scale, offset).astype(BF16)).astype(BF16)
        tok_scr[:, tok] = token
        normed = layer_norm(token.astype(F32))
        query = tdot(weights[1][0], normed).astype(BF16)
        key = tdot(weights[1][1], normed).astype(BF16)
        value = tdot(weights[1][2], normed).astype(BF16)
        val_scr[:, tok] = value
        for h in range(heads):
            query_scr[h, 0:head_dim, tok] = query[h * head_dim:(h + 1) * head_dim]
            key_scr[h, tok, :] = jnp.concatenate([key[h * head_dim:(h + 1) * head_dim], pad], axis=0).T
        return largest(query, carry[0]), largest(key, carry[1]), largest(value, carry[2])

    zero = jnp.zeros((heads, block), F32)
    norms = lax.fori_loop(0, tokens // block, project, (zero, zero, zero))
    query_norm, key_norm, value_norm = [jnp.max(norm, axis=1, keepdims=True) for norm in norms]
    logit_bound = jnp.max(query_norm * key_norm) / head_dim
    small = (logit_bound <= LOGIT_LIMIT ** 2) & (jnp.max(value_norm) <= VALUE_LIMIT ** 2)
    blocks, chunks = tokens // q_block, tokens // k_chunk

    def fold(combine, part):
        return combine(part.reshape(k_chunk // SUBLANES, SUBLANES, q_block), axis=0)

    def logits(h, cols, c):
        return jnp.dot(key_scr[h, c * k_chunk:(c + 1) * k_chunk, :], query_scr[h, :, cols], preferred_element_type=F32)

    def weigh(h, cols, slot, total):
        head = pl.ds(pl.multiple_of(h * head_dim, 16), head_dim)
        mixed = jnp.dot(val_scr[head, :], prob_scr[slot], preferred_element_type=F32)
        att_scr[head, cols] = (mixed * (1.0 / total)).astype(BF16)

    def attend(h, last_total):
        for b in range(blocks):
            cols = slice(b * q_block, (b + 1) * q_block)
            total = 0.0
            for c in range(chunks):
                prob = jnp.exp2(logits(h, cols, c) * exp_scale)
                total = total + fold(jnp.sum, prob)
                prob_scr[b % 2, c * k_chunk:(c + 1) * k_chunk, :] = prob.astype(BF16)
                if c == 1:
                    done = (b - 1) % blocks
                    weigh(h if b else jnp.maximum(h - 1, 0), slice(done * q_block, (done + 1) * q_block), done % 2, last_total)
            last_total = jnp.sum(total, axis=0, keepdims=True)
        return last_total

    @pl.when(small)
    def _():
        prob_scr[(blocks - 1) % 2] = jnp.zeros(prob_scr.shape[1:], BF16)
        total = lax.fori_loop(0, heads, attend, jnp.ones((1, q_block), F32))
        weigh(heads - 1, slice((blocks - 1) * q_block, blocks * q_block), (blocks - 1) % 2, total)

    @pl.when(jnp.logical_not(small))
    def _():
        def attend_shifted(i, carry):
            h = lax.div(i, blocks)
            cols = pl.ds(pl.multiple_of(lax.rem(i, blocks) * q_block, LANES), q_block)
            peak = None
            for c in range(chunks):
                part = logits(h, cols, c)
                logit_scr[c * k_chunk:(c + 1) * k_chunk, :] = part
                peak = fold(jnp.max, part) if peak is None else jnp.maximum(peak, fold(jnp.max, part))
            peak = jnp.max(peak, axis=0, keepdims=True)
            total = 0.0
            for c in range(chunks):
                prob = jnp.exp2((logit_scr[c * k_chunk:(c + 1) * k_chunk, :] - peak) * exp_scale)
                total = total + fold(jnp.sum, prob)
                prob_scr[0, c * k_chunk:(c + 1) * k_chunk, :] = prob.astype(BF16)
            weigh(h, cols, 0, jnp.sum(total, axis=0, keepdims=True))
            return carry

        lax.fori_loop(0, heads * blocks, attend_shifted, 0)

    ready(2, 3, 4, 5, 6, 7)
    text_pad = ctx_key_ref.shape[2]
    text_row = lax.broadcasted_iota(jnp.int32, (text_pad, block), 0)
    cross_pad = jnp.zeros((LANES - text_pad, block), BF16)

    def finish(i, carry):
        tok = pl.ds(pl.multiple_of(i * block, LANES), block)
        tok_one = (tok_scr[:, tok].astype(F32) + tdot(weights[2][...], att_scr[:, tok])).astype(BF16)
        query = tdot(weights[3][...], layer_norm(tok_one.astype(F32))).astype(BF16)
        for h in range(heads):
            head = slice(h * head_dim, (h + 1) * head_dim)
            logit = jnp.dot(ctx_key_ref[0, h], jnp.concatenate([query[head], pad], axis=0), preferred_element_type=F32)
            logit = jnp.where(text_row < text, logit, -jnp.inf)
            prob = jnp.exp2((logit - jnp.max(logit, axis=0, keepdims=True)) * exp_scale)
            total = jnp.sum(prob, axis=0, keepdims=True)
            mixed = jnp.dot(ctx_val_ref[0, head, :], jnp.concatenate([prob.astype(BF16), cross_pad], axis=0), preferred_element_type=F32)
            cross_scr[head, :] = (mixed * (1.0 / total)).astype(BF16)
        tok_two = (tok_one.astype(F32) + tdot(weights[4][...], cross_scr[...])).astype(BF16)
        normed = layer_norm(tok_two.astype(F32))
        chunk = channels
        for off in range(0, ff_width, chunk):
            value = tdot(weights[5][:, off:off + chunk], normed)
            gate = tdot(weights[5][:, ff_width + off:ff_width + off + chunk], normed)
            gate_scr[off:off + chunk, :] = (value * (0.5 * gate * (1.0 + lax.erf(gate * (0.5 ** 0.5))))).astype(BF16)
        tok_three = (tok_two.astype(F32) + tdot(weights[6][...], gate_scr[...])).astype(BF16)
        out = (hid_ref[0, :, tok].astype(F32) + tdot(weights[7][...], tok_three)).astype(BF16)
        out_ref[0, :, tok] = out
        out = out.astype(F32)
        return lane_sum(carry[0], out), lane_sum(carry[1], out * out)

    zero = jnp.zeros((channels, LANES), F32)
    sums, squares = lax.fori_loop(0, tokens // block, finish, (zero, zero))
    parts_ref[0, :, 0:LANES] = sums
    parts_ref[0, :, LANES:2 * LANES] = squares


def former(stacked, parts, cols, ctx_key, ctx_val, weights, text, group_width):
    images, channels, tokens = stacked.shape
    heads = ctx_key.shape[1]
    block, q_block, k_chunk = 512, 256, 256
    per_image = lambda a: pl.BlockSpec((1,) + a.shape[1:], lambda i: (i,) + (0,) * (a.ndim - 1))
    whole = lambda a: pl.BlockSpec(a.shape, lambda i: (0,) * a.ndim)
    ff_width = weights[6].shape[0]
    flops = 2 * images * tokens * (channels * channels * 8 + 3 * channels * ff_width + 2 * tokens * channels * 3)
    return pl.pallas_call(
        functools.partial(former_kernel, heads, text, group_width, block, q_block, k_chunk),
        grid=(images,),
        out_shape=(jax.ShapeDtypeStruct(stacked.shape, BF16), jax.ShapeDtypeStruct(parts.shape, F32)),
        in_specs=[per_image(stacked), per_image(parts), whole(cols), per_image(ctx_key), per_image(ctx_val)] + [pl.BlockSpec(memory_space=pltpu.HBM)] * len(weights),
        out_specs=(per_image(stacked), per_image(parts)),
        scratch_shapes=[
            pltpu.VMEM((channels, tokens), BF16), pltpu.VMEM((heads, LANES, tokens), BF16), pltpu.VMEM((heads, tokens, LANES), BF16),
            pltpu.VMEM((channels, tokens), BF16), pltpu.VMEM((channels, tokens), BF16),
            pltpu.VMEM((tokens, q_block), F32), pltpu.VMEM((2, tokens, q_block), BF16),
            pltpu.VMEM((channels, block), BF16), pltpu.VMEM((ff_width, block), BF16)]
        + [pltpu.VMEM(w.shape, BF16) for w in weights] + [pltpu.SemaphoreType.DMA((len(weights),))],
        name='former',
        cost_estimate=pl.CostEstimate(flops=flops, bytes_accessed=60 * MIB, transcendentals=0),
        compiler_params=pltpu.CompilerParams(vmem_limit_bytes=60 * MIB),
    )(stacked, parts, cols, ctx_key, ctx_val, *weights)


def time_project(time_emb, weight):
    time_act = jax.nn.silu(time_emb.astype(F32)).astype(BF16)
    return jnp.dot(time_act, weight, preferred_element_type=F32)


def solution(mesh):
    num_bands = mesh.shape['sp']

    def local_stage(latent, time_emb, context, res_conv, res_time, res_norm, attn_norm, proj_inout, self_qkv, self_out, cross_q, cross_kv, cross_out, ff_in, ff_out):
        batch, _, width, channels = latent.shape
        images = batch // num_bands
        tokens = num_bands * latent.shape[1] * width
        groups = res_norm.shape[3]
        heads, head_dim = self_out.shape[:2]
        text = context.shape[1]
        me = lax.axis_index('sp')

        def own(array):
            split = array.reshape((images, num_bands) + array.shape[1:])
            return lax.dynamic_index_in_dim(split, me, 1, keepdims=False)

        own_time, own_context = own(time_emb), own(context)
        norm_cols = res_norm.astype(F32).reshape(2, 4, channels)
        res_cols = []
        for i in range(2):
            shared = jnp.broadcast_to(norm_cols[i][None], (images, 4, channels))
            shared = jnp.concatenate([shared, time_project(own_time, res_time[i])[:, None, :]], axis=1)
            shared = jnp.pad(shared, ((0, 0), (0, groups - 5), (0, 0)))
            res_cols.append(jnp.swapaxes(shared, 1, 2))
        attn_cols = jnp.pad(attn_norm.astype(F32).reshape(2, channels), ((0, groups - 2), (0, 0))).T
        text_pad = -(-text // 16) * 16
        ctx_key = jnp.einsum('btc,chd->bhtd', own_context, cross_kv[0], preferred_element_type=F32).astype(BF16)
        ctx_key = jnp.pad(ctx_key, ((0, 0), (0, 0), (0, text_pad - text), (0, LANES - head_dim)))
        ctx_val = jnp.einsum('btc,chd->bhdt', own_context, cross_kv[1], preferred_element_type=F32).astype(BF16)
        ctx_val = jnp.pad(ctx_val.reshape(images, channels, text), ((0, 0), (0, 0), (0, LANES - text)))
        weights = (proj_inout[0], self_qkv.reshape(3, channels, channels), self_out.reshape(channels, channels), cross_q.reshape(channels, channels), cross_out.reshape(channels, channels), ff_in, ff_out, proj_inout[1])
        conv_weights = res_conv.reshape(4, 9 * channels, channels)

        group_width = channels // groups
        rows, received, later = latent, [], (ctx_key, ctx_val) + weights
        for i in range(images):
            if received:
                rows, later = lax.optimization_barrier((rows, later))
            received.append(lax.all_to_all(rows[i * num_bands:(i + 1) * num_bands], 'sp', 0, 1, tiled=True))
        ctx_key, ctx_val, *weights = later
        before = ()
        for i in range(images):
            before = res_block_in(i, images, received[i].reshape(tokens, channels), res_cols[0], conv_weights, 0, width, group_width, before)
        stacked, parts = former(*before, attn_cols, ctx_key, ctx_val, weights, text, group_width)
        out = res_block_out('sp', num_bands, stacked, parts, res_cols[1], conv_weights, 2, width, group_width)
        return out.reshape(latent.shape)

    band_spec = P('dp', 'sp', None, None)
    shared = P()
    in_specs = (band_spec, P('dp', None), P('dp', None, None)) + (shared,) * 12
    return jax.shard_map(local_stage, mesh=mesh, in_specs=in_specs, out_specs=band_spec, check_vma=False)
```

```python
import functools
import math
import jax
import jax.numpy as jnp
from jax import lax
from jax.experimental import pallas as pl
from jax.experimental.pallas import tpu as pltpu
from jax.sharding import PartitionSpec as P

GN_EPS = 1e-6
LN_EPS = 1e-5
LANES = 128
SUBLANES = 8
MESH = pl.DeviceIdType.MESH
LOGIT_LIMIT = 60.0
VALUE_LIMIT = 1e8
MIB = 2 ** 20
F32 = jnp.float32
BF16 = jnp.bfloat16
LHS_T = (((0,), (0,)), ((), ()))
BOTH_T = (((0,), (1,)), ((), ()))
LAST = (((1,), (1,)), ((), ()))


def tdot(weight, act):
    return lax.dot_general(weight, act, LHS_T, preferred_element_type=F32)


def lane_sum(parts, value):
    total = parts
    for off in range(0, value.shape[1], LANES):
        total = total + value[:, off:off + LANES]
    return total


def group_affine(sums, squares, width, count, gain, shift):
    span = math.lcm(width, SUBLANES)
    row = lax.broadcasted_iota(jnp.int32, (SUBLANES, LANES), 0)
    scales, offsets = [], []

    def group_mean(array, base, low, high):
        total = None
        for top in range(0, span, SUBLANES):
            first, last = max(low - top, 0), min(high - top, SUBLANES)
            if first < last:
                tile = array[base + top:base + top + SUBLANES]
                if last - first < SUBLANES:
                    tile = jnp.where((row >= first) & (row < last), tile, 0.0)
                total = tile if total is None else total + tile
        for turn in (4, 2, 1):
            total = total + pltpu.roll(total, turn, 0)
        return jnp.broadcast_to(jnp.sum(total, axis=1, keepdims=True), (SUBLANES, LANES)) / count

    for base in range(0, sums.shape[0], span):
        means, rstds = [], []
        for low in range(0, span, width):
            mean = group_mean(sums, base, low, low + width)
            means.append(mean)
            rstds.append(lax.rsqrt(group_mean(squares, base, low, low + width) - mean * mean + GN_EPS))
        for top in range(0, span, SUBLANES):
            mean, rstd = means[top // width], rstds[top // width]
            for nxt in range(top // width + 1, (top + SUBLANES - 1) // width + 1):
                mean = jnp.where(row >= nxt * width - top, means[nxt], mean)
                rstd = jnp.where(row >= nxt * width - top, rstds[nxt], rstd)
            here = slice(base + top, base + top + SUBLANES)
            scale = rstd * gain[here]
            scales.append(scale)
            offsets.append(shift[here] - mean * scale)
    return jnp.concatenate(scales, axis=0), jnp.concatenate(offsets, axis=0)


def affine(block, scale, offset):
    pieces = [block[:, off:off + LANES].astype(F32) * scale + offset for off in range(0, block.shape[1], LANES)]
    return jnp.concatenate(pieces, axis=1)


def layer_norm(tokens):
    centred = tokens - jnp.mean(tokens, axis=0, keepdims=True)
    return (centred * lax.rsqrt(jnp.mean(centred * centred, axis=0, keepdims=True) + LN_EPS)).astype(BF16)


def res_phase(which, first, width, group_width, hid, cols, cur, wide, aff, weight, sums, squares, conv_block, order, keep, emit):
    channels, tokens = cur.shape
    count = float(tokens * group_width)
    gain = jnp.where(first, cols[:, 0:1], cols[:, 2:3])
    shift = jnp.where(first, cols[:, 1:2], cols[:, 3:4])
    scale, offset = group_affine(sums, squares, group_width, count, gain, shift)
    aff[0], aff[1] = 0.5 * scale, 0.5 * offset
    act_block, edge = 2 * width, 16
    row = lax.broadcasted_iota(jnp.int32, (edge, channels), 0)

    def widen(i, carry):
        tok = pl.ds(pl.multiple_of(i * act_block, LANES), act_block)
        half = affine(cur[:, tok], aff[0], aff[1])
        act = (half + half * jnp.tanh(half)).T
        left, right = pltpu.roll(act, 1, 0), pltpu.roll(act, act_block - 1, 0)

        def put(tap, base, value):
            dst = pl.ds(pl.multiple_of(i * act_block + width + base, edge), value.shape[0])
            wide[dst, tap * channels:(tap + 1) * channels] = value.astype(BF16)

        put(1, 0, act)
        for base in range(0, act_block, width):
            put(0, base, jnp.where(row == 0, 0.0, left[base:base + edge]))
            put(0, base + edge, left[base + edge:base + width])
            put(2, base, right[base:base + width - edge])
            put(2, base + width - edge, jnp.where(row == edge - 1, 0.0, right[base + width - edge:base + width]))
        return carry

    lax.fori_loop(0, tokens // act_block, widen, 0)
    if weight[1] is not None:
        weight[1].wait()
    time_term = cols[:, 4:5]
    cut = -(-channels // LANES // 2) * LANES

    def convolve(i, carry):
        block = order(i)
        start = block * conv_block
        tok = pl.ds(pl.multiple_of(start, LANES), conv_block)
        taps_in = jnp.concatenate([wide[pl.ds(pl.multiple_of(start + dy * width, 64), conv_block), :] for dy in range(3)], axis=1)
        sums, squares = [], []
        for low, high in ((0, cut), (cut, channels)):
            value = lax.dot_general(weight[0][which, :, low:high], taps_in, BOTH_T, preferred_element_type=F32)
            out = value + jnp.where(first, time_term[low:high], hid[low:high, tok].astype(F32))
            cur[low:high, tok] = out.astype(BF16)
            keep(tok, low, high, out)
            out = out.astype(BF16).astype(F32)
            sums.append(lane_sum(carry[0][low:high], out))
            squares.append(lane_sum(carry[1][low:high], out * out))
        emit(block)
        return jnp.concatenate(sums, axis=0), jnp.concatenate(squares, axis=0)

    zero = jnp.zeros((channels, LANES), F32)
    return lax.fori_loop(0, tokens // conv_block, convolve, (zero, zero))


def clear_border(wide, width):
    rows, taps = wide.shape
    wide[0:width, :] = jnp.zeros((width, taps), BF16)
    wide[rows - width:rows, :] = jnp.zeros((width, taps), BF16)


def weight_copies(weight_hbm, weight_scr, sems, first_conv):
    return lambda i: pltpu.make_async_copy(weight_hbm.at[first_conv + i], weight_scr.at[i], sems.at[i])


def greet(axis, bands, me):
    barrier = pltpu.get_barrier_semaphore()
    for step in range(1, bands):
        pl.semaphore_signal(barrier, inc=1, device_id={axis: lax.rem(me + step, bands)}, device_id_type=MESH)
    return lambda: pl.semaphore_wait(barrier, bands - 1)


def entry_kernel(axis, bands, latent_hbm, time_ref, ctx_ref, norm_ref, time_w_hbm, ctx_w_hbm, first_hbm, cols_one_ref, cols_two_ref, key_ref, val_ref, time_scr, ctx_scr, send_sems, recv_sems, own_sems):
    me = lax.axis_index(axis)
    everyone_here = greet(axis, bands, me)

    def remote(peer, source):
        return pltpu.make_async_remote_copy(
            src_ref=latent_hbm.at[peer, 0], dst_ref=first_hbm.at[source],
            send_sem=send_sems.at[peer], recv_sem=recv_sems.at[source], device_id={axis: peer}, device_id_type=MESH)

    own = pltpu.make_async_copy(latent_hbm.at[me, 0], first_hbm.at[me], own_sems.at[0])
    everyone_here()
    for step in range(1, bands):
        remote(lax.rem(me + step, bands), me).start()
    loads = [pltpu.make_async_copy(time_w_hbm, time_scr, own_sems.at[1]), pltpu.make_async_copy(ctx_w_hbm, ctx_scr, own_sems.at[2])]
    own.start()
    for load in loads:
        load.start()
    images, heads, text_pad, _ = key_ref.shape
    channels = val_ref.shape[1]
    head_dim = channels // heads
    half = 0.5 * time_ref[...].astype(F32)
    time_act = (half + half * jnp.tanh(half)).astype(BF16)
    lane = lax.broadcasted_iota(jnp.int32, norm_ref.shape[1:], 1)
    loads[0].wait()
    for block, cols_ref in enumerate((cols_one_ref, cols_two_ref)):
        term = lax.dot_general(time_scr[block], time_act, BOTH_T, preferred_element_type=F32)
        place = lax.broadcasted_iota(jnp.int32, term.shape, 1)
        for j in range(images):
            mine = jnp.sum(jnp.where(place == j * bands + me, term, 0.0), axis=1, keepdims=True)
            cols_ref[j] = jnp.where(lane == 4, mine, norm_ref[block])
    loads[1].wait()
    pad = jnp.zeros((LANES - head_dim, LANES), BF16)
    for j in range(images):
        key = lax.dot_general(ctx_scr[0], ctx_ref[j], LAST, preferred_element_type=F32).astype(BF16)
        for h in range(heads):
            key_ref[j, h] = jnp.concatenate([key[h * head_dim:(h + 1) * head_dim], pad], axis=0).T[0:text_pad]
        val_ref[j] = lax.dot_general(ctx_scr[1], ctx_ref[j], LAST, preferred_element_type=F32).astype(BF16)
    for step in range(1, bands):
        peer = lax.rem(me + step, bands)
        remote(peer, me).wait_send()
        remote(peer, peer).wait_recv()
    own.wait()


def entry(axis, bands, images, heads, text_pad, latent, time_emb, own_context, norm_cols, time_w, ctx_w):
    _, _, width, channels = latent.shape
    vmem, hbm = pl.BlockSpec(memory_space=pltpu.VMEM), pl.BlockSpec(memory_space=pltpu.HBM)
    cols = jax.ShapeDtypeStruct((images,) + norm_cols.shape[1:], F32)
    return pl.pallas_call(
        functools.partial(entry_kernel, axis, bands),
        out_shape=(jax.ShapeDtypeStruct((bands, width, channels), BF16), cols, cols, jax.ShapeDtypeStruct((images, heads, text_pad, LANES), BF16), jax.ShapeDtypeStruct((images, channels, LANES), BF16)),
        in_specs=[hbm, vmem, vmem, vmem, hbm, hbm],
        out_specs=(hbm, vmem, vmem, vmem, vmem),
        scratch_shapes=[pltpu.VMEM(time_w.shape, BF16), pltpu.VMEM(ctx_w.shape, BF16), pltpu.SemaphoreType.DMA((bands,)), pltpu.SemaphoreType.DMA((bands,)), pltpu.SemaphoreType.DMA((3,))],
        name='entry',
        cost_estimate=pl.CostEstimate(flops=10 ** 9, bytes_accessed=8 * MIB, transcendentals=0),
        compiler_params=pltpu.CompilerParams(vmem_limit_bytes=60 * MIB, collective_id=8, has_side_effects=True),
    )(latent, time_emb, own_context, norm_cols, time_w, ctx_w)


def res_in_kernel(axis, bands, image, sending, width, group_width, first_conv, conv_block, hid_ref, cols_ref, weight_hbm, *refs):
    if sending:
        latent_hbm, (next_hbm, *refs), sync = refs[0], refs[-11:-3], refs[-3:]
        send_sems, recv_sems, own_sem = sync
        out_ref, parts_ref = refs[:2]
    out_ref, parts_ref, hid_scr, wide_scr, aff_scr, weight_scr, sems = refs[-7:]
    channels, tokens = hid_scr.shape
    copies = weight_copies(weight_hbm, weight_scr, sems, first_conv)
    for i in range(2):
        copies(i).start()
    if sending:
        me = lax.axis_index(axis)
        everyone_here = greet(axis, bands, me)
    clear_border(wide_scr, width)
    act_block = 2 * width
    cur = out_ref.at[0]

    def load(i, carry):
        tok = pl.ds(pl.multiple_of(i * act_block, LANES), act_block)
        block = hid_ref[tok, :].astype(F32).T
        hid_scr[:, tok] = block.astype(BF16)
        cur[:, tok] = block.astype(BF16)
        return lane_sum(carry[0], block), lane_sum(carry[1], block * block)

    zero = jnp.zeros((channels, LANES), F32)
    stats = lax.fori_loop(0, tokens // act_block, load, (zero, zero))

    if sending:
        def remote(peer, source):
            return pltpu.make_async_remote_copy(
                src_ref=latent_hbm.at[(image + 1) * bands + peer, 0], dst_ref=next_hbm.at[source],
                send_sem=send_sems.at[peer], recv_sem=recv_sems.at[source], device_id={axis: peer}, device_id_type=MESH)

        own = pltpu.make_async_copy(latent_hbm.at[(image + 1) * bands + me, 0], next_hbm.at[me], own_sem.at[0])
        everyone_here()
        for step in range(1, bands):
            remote(lax.rem(me + step, bands), me).start()
        own.start()

    def half(which, stats):
        return res_phase(which, which == 0, width, group_width, hid_scr, cols_ref[0], cur, wide_scr, aff_scr, (weight_scr, copies(which)), *stats, conv_block, lambda i: i, lambda *piece: None, lambda block: None)

    sums, squares = lax.fori_loop(0, 2, half, stats)
    parts_ref[0, :, 0:LANES] = sums
    parts_ref[0, :, LANES:2 * LANES] = squares
    if sending:
        for step in range(1, bands):
            peer = lax.rem(me + step, bands)
            remote(peer, me).wait_send()
            remote(peer, peer).wait_recv()
        own.wait()


def res_out_kernel(axis, bands, width, group_width, first_conv, conv_block, hid_hbm, parts_ref, cols_ref, weight_hbm, out_hbm, hid_ref, cur_scr, wide_scr, aff_scr, rows_scr, weight_scr, hid_sems, sems, send_sems, recv_sems, own_sems):
    images, channels, tokens = hid_ref.shape
    fetches = [pltpu.make_async_copy(hid_hbm.at[i], hid_ref.at[i], hid_sems.at[i]) for i in range(images)]
    for fetch in fetches:
        fetch.start()
    band = tokens // bands
    me = lax.axis_index(axis)
    copies = weight_copies(weight_hbm, weight_scr, sems, first_conv)
    for i in range(2):
        copies(i).start()
    everyone_here = greet(axis, bands, me)
    clear_border(wide_scr, width)
    everyone_here()
    for fetch in fetches:
        fetch.wait()

    blocks = tokens // conv_block
    stride = jnp.where(lax.rem(me, 2) == 0, 1, blocks - 1)

    def order(i):
        return lax.rem(lax.div(me * band, conv_block) + (i + 1) * stride, blocks)

    def remote(image, peer, source, low=0, high=band, to=None):
        to = peer if to is None else to
        return pltpu.make_async_remote_copy(
            src_ref=rows_scr.at[image, pl.ds(peer * band + low, high - low)], dst_ref=out_hbm.at[image * bands + source, pl.ds(low, high - low)],
            send_sem=send_sems.at[image, to], recv_sem=recv_sems.at[image, source], device_id={axis: to}, device_id_type=MESH)

    def local(image, peer, low=0, high=band):
        return pltpu.make_async_copy(rows_scr.at[image, pl.ds(peer * band + low, high - low)], out_hbm.at[image * bands + me, pl.ds(low, high - low)], own_sems.at[image])

    def per_image(image, carry):
        cur_scr[...] = hid_ref[image]

        def half(which, stats):
            def keep(tok, low, high, out):
                rows_scr[image, tok, low:high] = out.T.astype(BF16)

            def emit(block):
                for ready in range(tokens // conv_block):
                    for peer in range(bands):
                        low = max(ready * conv_block - peer * band, 0)
                        high = min((ready + 1) * conv_block - peer * band, band)
                        if low >= high:
                            continue
                        now = (which == 1) & (block == ready)

                        @pl.when(now & (me != peer))
                        def _():
                            remote(image, peer, me, low, high).start()

                        @pl.when(now & (me == peer))
                        def _():
                            local(image, peer, low, high).start()

            @pl.when((image == 0))
            def _():
                copies(which).wait()

            return res_phase(which, which == 0, width, group_width, hid_ref.at[image], cols_ref[image], cur_scr, wide_scr, aff_scr, (weight_scr, None), *stats, conv_block, order, keep, emit)

        lax.fori_loop(0, 2, half, (parts_ref[image, :, 0:LANES], parts_ref[image, :, LANES:2 * LANES]))
        return carry

    lax.fori_loop(0, images, per_image, 0)
    def settle(i, carry):
        image, peer = lax.div(i, bands - 1), lax.rem(me + 1 + lax.rem(i, bands - 1), bands)
        remote(image, 0, peer, to=peer).wait_recv()
        remote(image, 0, me, to=peer).wait_send()
        return carry

    lax.fori_loop(0, images * (bands - 1), settle, 0)
    for image in range(images):
        local(image, 0).wait()


def res_cost(images, channels, tokens):
    return pl.CostEstimate(flops=2 * 2 * 9 * images * channels * channels * tokens, bytes_accessed=40 * channels * channels, transcendentals=0)


def res_block_in(axis, bands, image, images, hid, latent, cols, weights, first_conv, width, group_width, before):
    tokens, channels = hid.shape
    conv_block, taps = 512, 3 * channels
    sending = image + 1 < images
    slot = lambda i: (image, 0, 0)
    any_spec, hbm = pl.BlockSpec(memory_space=pl.ANY), pl.BlockSpec(memory_space=pltpu.HBM)
    extra = (latent,) if sending else ()
    start = 3 + len(extra)
    received = (jax.ShapeDtypeStruct((bands, tokens // bands, channels), BF16),) if sending else ()
    params = dict(collective_id=1 + image, has_side_effects=True) if sending else {}
    result = pl.pallas_call(
        functools.partial(res_in_kernel, axis, bands, image, sending, width, group_width, first_conv, conv_block),
        grid=(1,),
        out_shape=received + (jax.ShapeDtypeStruct((images, channels, tokens), BF16), jax.ShapeDtypeStruct((images, channels, 2 * LANES), F32)),
        in_specs=[pl.BlockSpec(hid.shape, lambda i: (0, 0)), pl.BlockSpec((1,) + cols.shape[1:], slot), hbm] + [hbm] * len(extra) + [any_spec] * len(before),
        out_specs=(hbm,) * len(received) + (pl.BlockSpec((1, channels, tokens), slot), pl.BlockSpec((1, channels, 2 * LANES), slot)),
        scratch_shapes=[
            pltpu.VMEM((channels, tokens), BF16), pltpu.VMEM((tokens + 2 * width, taps), BF16),
            pltpu.VMEM((2, channels, LANES), F32), pltpu.VMEM((2, 3 * taps, channels), BF16), pltpu.SemaphoreType.DMA((2,))]
        + [pltpu.SemaphoreType.DMA((bands,)), pltpu.SemaphoreType.DMA((bands,)), pltpu.SemaphoreType.DMA((1,))] * sending,
        input_output_aliases={start + i: len(received) + i for i in range(len(before))},
        name='res_in',
        cost_estimate=res_cost(1, channels, tokens),
        compiler_params=pltpu.CompilerParams(vmem_limit_bytes=62 * MIB, **params),
    )(hid, cols, weights, *extra, *before)
    return (result[0] if sending else None), result[-2:]


def res_block_out(axis, bands, stacked, parts, cols, weights, first_conv, width, group_width):
    images, channels, tokens = stacked.shape
    conv_block, taps = 512, 3 * channels
    vmem = pl.BlockSpec(memory_space=pltpu.VMEM)
    return pl.pallas_call(
        functools.partial(res_out_kernel, axis, bands, width, group_width, first_conv, conv_block),
        out_shape=jax.ShapeDtypeStruct((images * bands, tokens // bands, channels), BF16),
        in_specs=[pl.BlockSpec(memory_space=pltpu.HBM), vmem, vmem, pl.BlockSpec(memory_space=pltpu.HBM)],
        out_specs=pl.BlockSpec(memory_space=pltpu.HBM),
        scratch_shapes=[
            pltpu.VMEM(stacked.shape, BF16), pltpu.VMEM((channels, tokens), BF16), pltpu.VMEM((tokens + 2 * width, taps), BF16),
            pltpu.VMEM((2, channels, LANES), F32), pltpu.VMEM((images, tokens, channels), BF16), pltpu.VMEM((2, 3 * taps, channels), BF16),
            pltpu.SemaphoreType.DMA((images,)), pltpu.SemaphoreType.DMA((2,)), pltpu.SemaphoreType.DMA((images, bands)), pltpu.SemaphoreType.DMA((images, bands)), pltpu.SemaphoreType.DMA((images,))],
        name='res_out',
        cost_estimate=res_cost(images, channels, tokens),
        compiler_params=pltpu.CompilerParams(vmem_limit_bytes=48 * MIB, collective_id=0, has_side_effects=True),
    )(stacked, parts, cols, weights)


def former_kernel(heads, text, group_width, block, q_block, k_chunk, hid_ref, part_in_ref, cols_ref, ctx_key_ref, ctx_val_ref, *refs):
    weights_hbm, refs = refs[:7], refs[7:]
    out_ref, parts_ref, tok_scr, query_scr, key_scr, val_scr, att_scr, logit_scr, prob_scr, cross_scr, gate_scr, two_scr, normed_scr = refs[:13]
    weights, sems = refs[13:20], refs[20]
    _, channels, tokens = hid_ref.shape
    head_dim = channels // heads
    ff_width = weights[6].shape[0]
    count = float(tokens * group_width)
    exp_scale = head_dim ** -0.5 * 1.4426950408889634
    first = pl.program_id(0) == 0
    copies = [pltpu.make_async_copy(weights_hbm[i], weights[i], sems.at[i]) for i in range(7)]

    @pl.when(first)
    def _():
        for copy in copies:
            copy.start()
        query_scr[...] = jnp.zeros(query_scr.shape, BF16)

    def ready(*which):
        @pl.when(first)
        def _():
            for i in which:
                copies[i].wait()

    scale, offset = group_affine(part_in_ref[0, :, 0:LANES], part_in_ref[0, :, LANES:2 * LANES], group_width, count, cols_ref[:, 0:1], cols_ref[:, 1:2])
    ready(0, 1)
    pad = jnp.zeros((query_scr.shape[1] - head_dim, block), BF16)

    split = block // 2

    def largest(value, before):
        square = value.astype(F32)
        square = (square * square).reshape(heads, head_dim, value.shape[1])
        return jnp.maximum(jnp.sum(square, axis=1), before)

    def project(i, carry):
        toks = [pl.ds(pl.multiple_of(i * block + off, LANES), split) for off in range(0, block, split)]
        tokens_in = [tdot(weights[0][0], affine(hid_ref[0, :, tok], scale, offset).astype(BF16)).astype(BF16) for tok in toks]
        normed = [layer_norm(token.astype(F32)) for token in tokens_in]
        for tok, token in zip(toks, tokens_in):
            tok_scr[:, tok] = token
        for tok, norm in zip(toks, normed):
            query = jnp.dot(weights[1][0], norm, preferred_element_type=F32).astype(BF16)
            key = jnp.dot(weights[1][1], norm, preferred_element_type=F32).astype(BF16)
            value = jnp.dot(weights[1][2], norm, preferred_element_type=F32).astype(BF16)
            val_scr[:, tok] = value
            for h in range(heads):
                query_scr[h, 0:head_dim, tok] = query[h * head_dim:(h + 1) * head_dim]
                key_scr[h, tok, :] = jnp.concatenate([key[h * head_dim:(h + 1) * head_dim], pad[:, 0:split]], axis=0).T
            carry = largest(query, carry[0]), largest(key, carry[1]), largest(value, carry[2])
        return carry

    zero = jnp.zeros((heads, split), F32)
    norms = lax.fori_loop(0, tokens // block, project, (zero, zero, zero))
    query_norm, key_norm, value_norm = [jnp.max(norm, axis=1, keepdims=True) for norm in norms]
    logit_bound = jnp.max(query_norm * key_norm) / head_dim
    small = (logit_bound <= LOGIT_LIMIT ** 2) & (jnp.max(value_norm) <= VALUE_LIMIT ** 2)
    blocks, chunks = tokens // q_block, tokens // k_chunk

    def fold(combine, part):
        return combine(part.reshape(k_chunk // SUBLANES, SUBLANES, q_block), axis=0)

    def logits(h, cols, c):
        return jnp.dot(key_scr[h, c * k_chunk:(c + 1) * k_chunk, :], query_scr[h, :, cols], preferred_element_type=F32)

    def weigh(h, cols, slot, total):
        head = pl.ds(pl.multiple_of(h * head_dim, 16), head_dim)
        mixed = jnp.dot(val_scr[head, :], prob_scr[slot], preferred_element_type=F32)
        att_scr[head, cols] = (mixed * (1.0 / total)).astype(BF16)

    def attend(h, last_total):
        for b in range(blocks):
            cols = slice(b * q_block, (b + 1) * q_block)
            total = 0.0
            for c in range(chunks):
                prob = jnp.exp2(logits(h, cols, c) * exp_scale)
                total = total + fold(jnp.sum, prob)
                prob_scr[b % 2, c * k_chunk:(c + 1) * k_chunk, :] = prob.astype(BF16)
                if c == 1:
                    done = (b - 1) % blocks
                    weigh(h if b else jnp.maximum(h - 1, 0), slice(done * q_block, (done + 1) * q_block), done % 2, last_total)
            last_total = jnp.sum(total, axis=0, keepdims=True)
        return last_total

    @pl.when(small)
    def _():
        prob_scr[(blocks - 1) % 2] = jnp.zeros(prob_scr.shape[1:], BF16)
        total = lax.fori_loop(0, heads, attend, jnp.ones((1, q_block), F32))
        weigh(heads - 1, slice((blocks - 1) * q_block, blocks * q_block), (blocks - 1) % 2, total)

    @pl.when(jnp.logical_not(small))
    def _():
        def attend_shifted(i, carry):
            h = lax.div(i, blocks)
            cols = pl.ds(pl.multiple_of(lax.rem(i, blocks) * q_block, LANES), q_block)
            peak = None
            for c in range(chunks):
                part = logits(h, cols, c)
                logit_scr[c * k_chunk:(c + 1) * k_chunk, :] = part
                peak = fold(jnp.max, part) if peak is None else jnp.maximum(peak, fold(jnp.max, part))
            peak = jnp.max(peak, axis=0, keepdims=True)
            total = 0.0
            for c in range(chunks):
                prob = jnp.exp2((logit_scr[c * k_chunk:(c + 1) * k_chunk, :] - peak) * exp_scale)
                total = total + fold(jnp.sum, prob)
                prob_scr[0, c * k_chunk:(c + 1) * k_chunk, :] = prob.astype(BF16)
            weigh(h, cols, 0, jnp.sum(total, axis=0, keepdims=True))
            return carry

        lax.fori_loop(0, heads * blocks, attend_shifted, 0)

    ready(2, 3, 4, 5, 6)
    text_pad = ctx_key_ref.shape[2]
    text_row = lax.broadcasted_iota(jnp.int32, (text_pad, block), 0)
    cross_pad = jnp.zeros((LANES - text_pad, block), BF16)

    def finish(i, carry):
        start = pl.multiple_of(i * block, LANES)
        tok = pl.ds(start, block)
        split = block // 2
        halves = [slice(off, off + split) for off in range(0, block, split)]
        toks = [pl.ds(pl.multiple_of(start + half.start, LANES), split) for half in halves]
        ones = [(tok_scr[:, t].astype(F32) + tdot(weights[2][...], att_scr[:, t])).astype(BF16) for t in toks]
        queries = [jnp.dot(weights[3][...], layer_norm(one.astype(F32)), preferred_element_type=F32).astype(BF16) for one in ones]
        for h in range(heads):
            head = slice(h * head_dim, (h + 1) * head_dim)
            for half, query in zip(halves, queries):
                logit = jnp.dot(ctx_key_ref[0, h], jnp.concatenate([query[head], pad[:, half]], axis=0), preferred_element_type=F32)
                logit = jnp.where(text_row[:, half] < text, logit, -jnp.inf)
                prob = jnp.exp2((logit - jnp.max(logit, axis=0, keepdims=True)) * exp_scale)
                total = jnp.sum(prob, axis=0, keepdims=True)
                mixed = jnp.dot(ctx_val_ref[0, head, :], jnp.concatenate([prob.astype(BF16), cross_pad[:, half]], axis=0), preferred_element_type=F32)
                cross_scr[head, half] = (mixed * (1.0 / total)).astype(BF16)
        for half, one in zip(halves, ones):
            two = (one.astype(F32) + tdot(weights[4][...], cross_scr[:, half])).astype(BF16)
            two_scr[:, half] = two
            normed_scr[:, half] = layer_norm(two.astype(F32))
        normed = normed_scr[...]
        chunk = channels
        for off in range(0, ff_width, chunk):
            value = tdot(weights[5][:, off:off + chunk], normed)
            gate = tdot(weights[5][:, ff_width + off:ff_width + off + chunk], normed)
            gate_scr[off:off + chunk, :] = (value * (0.5 * gate * (1.0 + lax.erf(gate * (0.5 ** 0.5))))).astype(BF16)
        tok_three = (two_scr[...].astype(F32) + tdot(weights[6][...], gate_scr[...])).astype(BF16)
        out = (hid_ref[0, :, tok].astype(F32) + tdot(weights[0][1], tok_three)).astype(BF16)
        out_ref[0, :, tok] = out
        out = out.astype(F32)
        return lane_sum(carry[0], out), lane_sum(carry[1], out * out)

    zero = jnp.zeros((channels, LANES), F32)
    sums, squares = lax.fori_loop(0, tokens // block, finish, (zero, zero))
    parts_ref[0, :, 0:LANES] = sums
    parts_ref[0, :, LANES:2 * LANES] = squares


def former(stacked, parts, cols, ctx_key, ctx_val, weights, text, group_width):
    images, channels, tokens = stacked.shape
    heads = ctx_key.shape[1]
    block, q_block, k_chunk = 512, 256, 256
    per_image = lambda a: pl.BlockSpec((1,) + a.shape[1:], lambda i: (i,) + (0,) * (a.ndim - 1))
    whole = lambda a: pl.BlockSpec(a.shape, lambda i: (0,) * a.ndim)
    ff_width = weights[6].shape[0]
    flops = 2 * images * tokens * (channels * channels * 8 + 3 * channels * ff_width + 2 * tokens * channels * 3)
    return pl.pallas_call(
        functools.partial(former_kernel, heads, text, group_width, block, q_block, k_chunk),
        grid=(images,),
        out_shape=(jax.ShapeDtypeStruct(stacked.shape, BF16), jax.ShapeDtypeStruct(parts.shape, F32)),
        in_specs=[per_image(stacked), per_image(parts), whole(cols), per_image(ctx_key), per_image(ctx_val)] + [pl.BlockSpec(memory_space=pltpu.HBM)] * len(weights),
        out_specs=(per_image(stacked), per_image(parts)),
        scratch_shapes=[
            pltpu.VMEM((channels, tokens), BF16), pltpu.VMEM((heads, LANES, tokens), BF16), pltpu.VMEM((heads, tokens, LANES), BF16),
            pltpu.VMEM((channels, tokens), BF16), pltpu.VMEM((channels, tokens), BF16),
            pltpu.VMEM((tokens, q_block), F32), pltpu.VMEM((2, tokens, q_block), BF16),
            pltpu.VMEM((channels, block), BF16), pltpu.VMEM((ff_width, block), BF16), pltpu.VMEM((channels, block), BF16), pltpu.VMEM((channels, block), BF16)]
        + [pltpu.VMEM(w.shape, BF16) for w in weights] + [pltpu.SemaphoreType.DMA((len(weights),))],
        name='former',
        cost_estimate=pl.CostEstimate(flops=flops, bytes_accessed=60 * MIB, transcendentals=0),
        compiler_params=pltpu.CompilerParams(vmem_limit_bytes=60 * MIB),
    )(stacked, parts, cols, ctx_key, ctx_val, *weights)


def solution(mesh):
    num_bands = mesh.shape['sp']

    def local_stage(latent, time_emb, context, res_conv, res_time, res_norm, attn_norm, proj_inout, self_qkv, self_out, cross_q, cross_kv, cross_out, ff_in, ff_out):
        batch, _, width, channels = latent.shape
        images = batch // num_bands
        tokens = num_bands * latent.shape[1] * width
        groups = res_norm.shape[3]
        heads, head_dim = self_out.shape[:2]
        text = context.shape[1]
        me = lax.axis_index('sp')

        def own(array):
            split = array.reshape((images, num_bands) + array.shape[1:])
            return lax.dynamic_index_in_dim(split, me, 1, keepdims=False)

        group_width = channels // groups
        text_pad = -(-text // 16) * 16
        own_context = jnp.pad(own(context), ((0, 0), (0, LANES - text), (0, 0)))
        norm_cols = jnp.swapaxes(jnp.pad(res_norm.astype(F32).reshape(2, 4, channels), ((0, 0), (0, 4), (0, 0))), 1, 2)
        attn_cols = jnp.pad(attn_norm.astype(F32).reshape(2, channels), ((0, 6), (0, 0))).T
        ctx_w = jnp.transpose(cross_kv, (0, 2, 3, 1)).reshape(2, channels, context.shape[2])
        rows, *res_cols, ctx_key, ctx_val = entry('sp', num_bands, images, heads, text_pad, latent, time_emb, own_context, norm_cols, res_time, ctx_w)
        weights = (proj_inout, jnp.transpose(self_qkv, (0, 2, 3, 1)).reshape(3, channels, channels), self_out.reshape(channels, channels), jnp.transpose(cross_q, (1, 2, 0)).reshape(channels, channels), cross_out.reshape(channels, channels), ff_in, ff_out)
        conv_weights = res_conv.reshape(4, 9 * channels, channels)
        before = ()
        for i in range(images):
            rows, before = res_block_in('sp', num_bands, i, images, rows.reshape(tokens, channels), latent, res_cols[0], conv_weights, 0, width, group_width, before)
        stacked, parts = former(*before, attn_cols, ctx_key, ctx_val, weights, text, group_width)
        out = res_block_out('sp', num_bands, stacked, parts, res_cols[1], conv_weights, 2, width, group_width)
        return out.reshape(latent.shape)

    band_spec = P('dp', 'sp', None, None)
    shared = P()
    in_specs = (band_spec, P('dp', None), P('dp', None, None)) + (shared,) * 12
    return jax.shard_map(local_stage, mesh=mesh, in_specs=in_specs, out_specs=band_spec, check_vma=False)
```
